32 devices in a mesh: path: 8 (over y, x, core), mod: 4 (over z).
Axes of the slice: x: 2, y: 2, z: 4, core: 2. Of those that a mesh axis runs over, the one named last changes fastest.
Arguments:
- activations: bfloat16 [8, 512, 4096], P('path', 'mod'), may hold values from -6 to 6
- cotangent: bfloat16 [8, 512, 4096], P('path', 'mod'), may hold values from -6 to 6
- first_weight: bfloat16 [8, 4096, 4096], P('path', None, 'mod'), may hold values from -6 to 6
- second_weight: bfloat16 [8, 4096, 4096], P('path', None, 'mod'), may hold values from -6 to 6
- first_master: float32 [4, 4096, 4096], P(None, ('path', 'mod')), may hold values from -6 to 6
- second_master: float32 [4, 4096, 4096], P(None, ('path', 'mod')), may hold values from -6 to 6
- first_moment: float32 [4, 4096, 4096], P(None, ('path', 'mod')), may hold values from -3 to 3
- second_moment: float32 [4, 4096, 4096], P(None, ('path', 'mod')), may hold values from -3 to 3
- routing: int32 [8, 2], replicated, may hold values from 0 to 3, as said below
Outputs:
- first_result: bfloat16 [8, 4096, 4096], P('path', None, 'mod')
- second_result: bfloat16 [8, 4096, 4096], P('path', None, 'mod')
The draws below stay inside these ranges and needn't reach their ends.
Inputs may be any that keep to these rules, and one draw needn't show every extreme that they name: `routing`: for each of the two levels, every one of the 4 modules is taken by at least one path.
All inputs are finite; a program needn't handle non-finite values.
Results may differ from the reference program's by a relative error of at most 0.0045.
Values may be sent and summed in bfloat16 or wider, within the bound.
A program may use at most 192 MiB of HBM per device.

```python
import jax
import jax.numpy as jnp
from jax import lax

D = 4096
MODS = 4
TOK = 512
PATHS = 8


def draw_routing(key, part):
    subkeys = jax.random.split(jax.random.fold_in(key, 17), 4)
    columns = []
    for level_index in range(2):
        picked = jax.random.randint(subkeys[level_index], (PATHS,), 0, MODS)
        shuffled = jax.random.permutation(subkeys[level_index + 2], PATHS)
        picked = picked.at[shuffled[:MODS]].set(jnp.arange(MODS))
        columns.append(picked)
    return jnp.stack(columns, axis=1).astype(jnp.int32)


def block_levels(key, dims, pieces, least, high):
    def one(axis_at, parts):
        steps = jax.random.uniform(jax.random.fold_in(jax.random.fold_in(key, 6), axis_at), (parts,), jnp.float32, least / len(pieces), high / len(pieces))
        return jnp.repeat(jnp.exp(steps), dims[axis_at] // parts).reshape((-1,) + (1,) * (len(dims) - axis_at - 1))

    loudness = one(*pieces[0])
    for cut in pieces[1:]:
        loudness = loudness * one(*cut)
    return loudness


def bell_draw(own_key, shape, deviation, most, cuts=(), dtype=jnp.bfloat16):
    level = block_levels(own_key, shape, cuts, -0.22, 0.18) if cuts else 1.0
    entries = jax.random.normal(own_key, shape, jnp.float32) * deviation * level
    return jnp.minimum(jnp.maximum(entries, -most), most).astype(dtype)


def setup_inputs(seed: int = 0) -> dict:
    keys = jax.random.split(jax.random.key(seed), 10)
    return {
        "activations": bell_draw(keys[0], (PATHS, TOK, D), 1.0, 6.0, ((0, 8), (1, 4))),
        "cotangent": bell_draw(keys[1], (PATHS, TOK, D), 1.0, 6.0, ((0, 8), (1, 4))),
        "first_weight": bell_draw(keys[2], (PATHS, D, D), 1.0, 6.0, ((0, 8), (2, 4))),
        "second_weight": bell_draw(keys[3], (PATHS, D, D), 1.0, 6.0, ((0, 8), (2, 4))),
        "first_master": bell_draw(keys[4], (MODS, D, D), 1.0, 6.0, ((1, 32),), jnp.float32),
        "second_master": bell_draw(keys[5], (MODS, D, D), 1.0, 6.0, ((1, 32),), jnp.float32),
        "first_moment": bell_draw(keys[6], (MODS, D, D), 0.5, 3.0, ((1, 32),), jnp.float32),
        "second_moment": bell_draw(keys[7], (MODS, D, D), 0.5, 3.0, ((1, 32),), jnp.float32),
        "routing": draw_routing(jax.random.fold_in(keys[9], 71), 0),
    }


inner_rate = 1.0
outer_rate = 0.7
momentum_decay = 0.9


def path_update(operands):
    inputs_full, upstream, weight_in, weight_out = operands
    scale = D ** -0.5
    pre = jnp.dot(inputs_full, weight_in, preferred_element_type=jnp.float32) * scale
    hidden = jax.nn.silu(pre).astype(jnp.bfloat16)
    grad_hidden = jnp.dot(upstream, weight_out, preferred_element_type=jnp.float32) * scale
    grad_out = lax.dot_general(upstream, hidden, (((0,), (0,)), ((), ())), preferred_element_type=jnp.float32) * scale
    sigma = jax.nn.sigmoid(pre)
    grad_pre = (grad_hidden * sigma * (1.0 + pre * (1.0 - sigma))).astype(jnp.bfloat16)
    grad_in = lax.dot_general(inputs_full, grad_pre, (((0,), (0,)), ((), ())), preferred_element_type=jnp.float32) * scale
    trained_in = (weight_in.astype(jnp.float32) - inner_rate * grad_in).astype(jnp.bfloat16)
    trained_out = (weight_out.astype(jnp.float32) - inner_rate * grad_out).astype(jnp.bfloat16)
    return trained_in, trained_out


def reference(activations, cotangent, first_weight, second_weight, first_master, second_master, first_moment, second_moment, routing):
    trained_in, trained_out = lax.map(path_update, (activations, cotangent, first_weight, second_weight))
    module_ids = jnp.arange(MODS).astype(jnp.int32)
    results = []
    levels = ((trained_in, first_master, first_moment), (trained_out, second_master, second_moment))
    for level_index in range(2):
        trained, master, moment = levels[level_index]
        onehot = (routing[:, level_index][:, None] == module_ids[None, :]).astype(jnp.float32)

        def accumulate(summed, operands):
            weights_row, trained_one = operands
            return summed + weights_row[:, None, None] * trained_one.astype(jnp.float32)[None], None

        summed, _ = lax.scan(accumulate, jnp.zeros(master.shape, jnp.float32), (onehot, trained))
        path_total = jnp.sum(onehot, axis=0)[:, None, None]
        outer = master - summed / path_total
        moment_new = momentum_decay * moment + outer
        renewed = (master - outer_rate * (outer + momentum_decay * moment_new)).astype(jnp.bfloat16)
        results.append(renewed[routing[:, level_index]])
    return results[0], results[1]
```

```python
import functools

import jax
import jax.numpy as jnp
from jax import lax
from jax.experimental import pallas as pl
from jax.experimental.pallas import tpu as pltpu
from jax.sharding import PartitionSpec as P

inner_rate = 1.0
outer_rate = 0.7
momentum_decay = 0.9

mean_factor = outer_rate * (1.0 + momentum_decay)
master_factor = 1.0 - mean_factor
moment_factor = -outer_rate * momentum_decay * momentum_decay

ANY = pl.BlockSpec(memory_space=pl.ANY)


def remote(src, dst, send_sem, recv_sem, where):
    return pltpu.make_async_remote_copy(
        src_ref=src,
        dst_ref=dst,
        send_sem=send_sem,
        recv_sem=recv_sem,
        device_id=where,
        device_id_type=pl.DeviceIdType.MESH,
    )


def run_all(copies):
    for copy in copies:
        copy.start()
    for copy in copies:
        copy.wait()


def scatter_kernel(
    paths, groups, t0, t1, b0, b1, a0, a1, c0, c1, send, recv, zsend, zrecv, local
):
    p = lax.axis_index("path")
    z = lax.axis_index("mod")
    rows = a0.shape[1]
    owned = b0.shape[1]
    columns = a0.shape[2]
    copies = []
    locals_ = []
    for level, (t, a) in enumerate(((t0, a0), (t1, a1))):
        own = t.at[pl.ds(p * rows, rows), :]
        locals_.append(pltpu.make_async_copy(own, a.at[p], local.at[level]))
    for level, (b, c) in enumerate(((b0, c0), (b1, c1))):
        own = b.at[:, :, pl.ds(pl.multiple_of(z * columns, columns), columns)]
        locals_.append(
            pltpu.make_async_copy(own, c.at[:, pl.ds(z * owned, owned), :], local.at[2 + level])
        )
    for level, (b, c) in enumerate(((b0, c0), (b1, c1))):
        for step in range(1, groups):
            to = lax.rem(z + step, groups)
            copies.append(
                remote(
                    b.at[:, :, pl.ds(pl.multiple_of(to * columns, columns), columns)],
                    c.at[:, pl.ds(z * owned, owned), :],
                    zsend.at[level, step],
                    zrecv.at[level, step],
                    (p, to),
                )
            )
    order = []
    for level, (t, a) in enumerate(((t0, a0), (t1, a1))):
        for step in range(paths - 1, 0, -1):
            to = lax.rem(p + step, paths)
            order.append(
                remote(
                    t.at[pl.ds(to * rows, rows), :],
                    a.at[p],
                    send.at[level, step],
                    recv.at[level, step],
                    (to, z),
                )
            )
    run_all(order + copies + locals_)


def scatter(t0, t1, b0, b1):
    paths = lax.axis_size("path")
    groups = lax.axis_size("mod")
    depth, columns = t0.shape
    modules = b0.shape[0]
    rows = depth // paths
    arrived = jax.ShapeDtypeStruct((paths, rows, columns), t0.dtype)
    base = jax.ShapeDtypeStruct((modules, rows, columns), b0.dtype)
    dma = pltpu.SemaphoreType.DMA
    return pl.pallas_call(
        functools.partial(scatter_kernel, paths, groups),
        out_shape=(arrived, arrived, base, base),
        in_specs=[ANY] * 4,
        out_specs=[ANY] * 4,
        scratch_shapes=[dma((2, paths)), dma((2, paths)), dma((2, groups)), dma((2, groups)), dma((4,))],
        compiler_params=pltpu.CompilerParams(has_side_effects=True),
        name="scatter",
    )(t0, t1, b0, b1)


def gather_kernel(paths, v0, v1, r0, r1, send, recv, local):
    p = lax.axis_index("path")
    z = lax.axis_index("mod")
    rows = v0.shape[1]
    copies = []
    locals_ = []
    for level, (v, r) in enumerate(((v0, r0), (v1, r1))):
        mine = r.at[pl.ds(p * rows, rows), :]
        locals_.append(pltpu.make_async_copy(v.at[p], mine, local.at[level]))
        for step in range(paths - 1, 0, -1):
            to = lax.rem(p + step, paths)
            copies.append(
                remote(v.at[to], mine, send.at[level, step], recv.at[level, step], (to, z))
            )
    run_all(copies + locals_)


def gather(v0, v1):
    paths, rows, columns = v0.shape
    result = jax.ShapeDtypeStruct((paths * rows, columns), v0.dtype)
    dma = pltpu.SemaphoreType.DMA
    return pl.pallas_call(
        functools.partial(gather_kernel, paths),
        out_shape=(result, result),
        in_specs=[ANY] * 2,
        out_specs=[ANY] * 2,
        scratch_shapes=[dma((2, paths)), dma((2, paths)), dma((2,))],
        compiler_params=pltpu.CompilerParams(has_side_effects=True),
        name="gather",
    )(v0, v1)


def combine_kernel(level, routing, factor, arrived, base, out, total, fresh):
    paths = arrived.shape[0]
    modules = base.shape[0]
    total[...] = jnp.zeros_like(total)
    for q in range(paths):
        m = routing[q, level]
        total[m] = total[m] + arrived[q].astype(jnp.float32)
    for m in range(modules):
        fresh[m] = (base[m].astype(jnp.float32) + factor[level, m] * total[m]).astype(out.dtype)
    for q in range(paths):
        out[q] = fresh[routing[q, level]]


def combine(level, routing, factor, arrived, base):
    paths, rows, columns = arrived.shape
    modules = base.shape[0]
    block = min(rows, 64)
    smem = pl.BlockSpec(memory_space=pltpu.SMEM)
    return pl.pallas_call(
        functools.partial(combine_kernel, level),
        grid=(rows // block,),
        out_shape=jax.ShapeDtypeStruct(arrived.shape, arrived.dtype),
        in_specs=[
            smem,
            smem,
            pl.BlockSpec((paths, block, columns), lambda i: (0, i, 0)),
            pl.BlockSpec((modules, block, columns), lambda i: (0, i, 0)),
        ],
        out_specs=pl.BlockSpec((paths, block, columns), lambda i: (0, i, 0)),
        scratch_shapes=[
            pltpu.VMEM((modules, block, columns), jnp.float32),
            pltpu.VMEM((modules, block, columns), arrived.dtype),
        ],
        name=f"combine_{level}",
    )(routing, factor, arrived, base)


def body(
    activations,
    cotangent,
    first_weight,
    second_weight,
    first_master,
    second_master,
    first_moment,
    second_moment,
    routing,
):
    inputs_full = lax.all_gather(activations, "mod", axis=1, tiled=True)[0]
    upstream = lax.all_gather(cotangent, "mod", axis=1, tiled=True)[0]

    def base_of(master, moment):
        return (master_factor * master + moment_factor * moment).astype(jnp.bfloat16)

    base_first = base_of(first_master, first_moment)
    base_second = base_of(second_master, second_moment)
    weight_in = first_weight[0]
    weight_out = second_weight[0]
    scale = inputs_full.shape[1] ** (-0.5)
    pre = jnp.dot(inputs_full, weight_in, preferred_element_type=jnp.float32) * scale
    hidden = jax.nn.silu(pre).astype(jnp.bfloat16)
    grad_hidden = jnp.dot(upstream, weight_out, preferred_element_type=jnp.float32) * scale
    grad_out = (
        lax.dot_general(
            upstream, hidden, (((0,), (0,)), ((), ())), preferred_element_type=jnp.float32
        )
        * scale
    )
    trained_out = (weight_out.astype(jnp.float32) - inner_rate * grad_out).astype(jnp.bfloat16)
    sigma = jax.nn.sigmoid(pre)
    grad_pre = (grad_hidden * sigma * (1.0 + pre * (1.0 - sigma))).astype(jnp.bfloat16)
    grad_in = (
        lax.dot_general(
            inputs_full, grad_pre, (((0,), (0,)), ((), ())), preferred_element_type=jnp.float32
        )
        * scale
    )
    trained_in = (weight_in.astype(jnp.float32) - inner_rate * grad_in).astype(jnp.bfloat16)

    arrived_first, arrived_second, own_first, own_second = scatter(
        trained_in, trained_out, base_first, base_second
    )
    modules = first_master.shape[0]
    taken = jnp.sum(
        (jnp.transpose(routing)[:, :, None] == jnp.arange(modules)).astype(jnp.float32), axis=1
    )
    factor = mean_factor / taken
    fresh_first = combine(0, routing, factor, arrived_first, own_first)
    fresh_second = combine(1, routing, factor, arrived_second, own_second)
    first_back, second_back = gather(fresh_first, fresh_second)
    return (first_back[None], second_back[None])


def solution(mesh):
    return jax.shard_map(
        body,
        mesh=mesh,
        in_specs=(
            P("path", "mod", None),
            P("path", "mod", None),
            P("path", None, "mod"),
            P("path", None, "mod"),
            P(None, ("path", "mod"), None),
            P(None, ("path", "mod"), None),
            P(None, ("path", "mod"), None),
            P(None, ("path", "mod"), None),
            P(),
        ),
        out_specs=(P("path", None, "mod"), P("path", None, "mod")),
        check_vma=False,
    )
```
